256 devices in a mesh: dp: 16 (over x, y_lo, core), blk: 16 (over y_hi, z).
Axes of the slice: x: 4, y: 4 (y_hi: 2, y_lo: 2; y = y_hi * 2 + y_lo), z: 8, core: 2. Of those that a mesh axis runs over, the one named last changes fastest.
Arguments:
- layer_input: bfloat16 [16, 4096, 2048], P('dp', 'blk'), may hold values from -6 to 6
- queries: bfloat16 [16, 4096, 1024], P('dp', 'blk'), may hold values from -28 to 28
- key_rows: bfloat16 [16, 4096, 1024], P('dp', 'blk'), may hold values from -4 to 4
- value_rows: bfloat16 [16, 4096, 1024], P('dp', 'blk'), may hold values from -6 to 6
- context: bfloat16 [16, 4096, 1024], P('dp', 'blk'), may hold values from -6 to 6
- grad_context: bfloat16 [16, 4096, 1024], P('dp', 'blk'), may hold values from -6 to 6
- grad_output: bfloat16 [16, 4096, 2048], P('dp', 'blk'), may hold values from -6 to 6
- earlier_mass: float32 [16, 4, 4096], P('dp', None, 'blk'), may hold values from 3 to 7
- grad_queries: float32 [16, 4096, 1024], P('dp', 'blk'), may hold values from -0.12 to 0.12
- grad_keys: float32 [16, 4096, 1024], P('dp', 'blk'), may hold values from -0.12 to 0.12
- grad_values: float32 [16, 4096, 1024], P('dp', 'blk'), may hold values from -0.12 to 0.12
- documents: int32 [16, 4096], P('dp', 'blk'), may hold values from 0 to 2, as said below
- weights: float32 [4, 2048, 1024], P(None, 'blk', 'dp'), may hold values from -0.125 to 0.125
- row_factor: float32 [4, 2048], P(None, 'blk'), may hold values from 1.525879e-08 to 1.5258789e-05
- column_factor: float32 [4, 1024], P(None, 'dp'), may hold values from 1.525879e-08 to 1.5258789e-05
Outputs:
- new_weights: float32 [4, 2048, 1024], P(None, 'blk', 'dp')
- new_row_factor: float32 [4, 2048], P(None, 'blk')
- new_column_factor: float32 [4, 1024], P(None, 'dp')
The draws below stay inside these ranges and needn't reach their ends.
Inputs may be any that keep to these rules, and one draw needn't show every extreme that they name: Read in order of position, a sequence's document numbers never fall; each sequence has three documents of 512 positions or more.
All inputs are finite; a program needn't handle non-finite values.
Results may differ from the reference program's by a relative error of at most 0.022.
Values may be sent and summed in bfloat16 or wider, within the bound.
A program may use at most 128 MiB of HBM per device.

```python
import math
import jax
import jax.numpy as jnp
from jax import lax

D = 2048
H = 4
TOK_DEV = 256
HH = 1024
LEN = 4096
BATCH = 16
N_BLK = 16


def folded_order(blocks, row_count):
    half = row_count // 2
    block_ids = jnp.arange(blocks, dtype=jnp.int32)[:, None]
    local = jnp.arange(row_count, dtype=jnp.int32)[None, :]
    lower = block_ids * half + local
    upper = (2 * blocks - 1 - block_ids) * half + local - half
    return jnp.where(local < half, lower, upper).reshape(-1)


def draw_documents(key, part):
    blocks = LEN // TOK_DEV
    order = folded_order(blocks, TOK_DEV)
    first_cut = jax.random.randint(jax.random.fold_in(key, 11), (BATCH, 1), LEN // 8, LEN // 2)
    second_cut = jax.random.randint(jax.random.fold_in(key, 12), (BATCH, 1), LEN // 2 + LEN // 8, LEN - LEN // 8 + 1)
    return (order[None, :] >= first_cut).astype(jnp.int32) + (order[None, :] >= second_cut).astype(jnp.int32)


def draw_pair(key):
    key_draw = jnp.clip(jax.random.normal(jax.random.fold_in(key, 21), (BATCH, LEN, HH), jnp.float32), -4.0, 4.0)
    query_draw = jnp.clip(jax.random.normal(jax.random.fold_in(key, 22), (BATCH, LEN, HH), jnp.float32), -4.0, 4.0)
    return (key_draw, query_draw)


def draw_key_rows(key, part):
    return draw_pair(key)[0].astype(jnp.bfloat16)


def draw_queries(key, part):
    return draw_pair(key)[1].astype(jnp.bfloat16)


def spiked(array, key, source, target, blocks, factor):
    def block_of(position):
        return (jnp.arange(array.shape[position]) // (array.shape[position] // blocks)).reshape((-1,) + (1,) * (array.ndim - 1 - position))

    near = jax.random.permutation(key, blocks)[block_of(target)]
    far = (block_of(target) + blocks // 2) % blocks
    return jnp.where((block_of(source) == near) | (block_of(source) == far), factor * array, array)


def shard_levels(key, extent, shards, least, largest):
    def one(position, shards_of):
        draws = jax.random.uniform(jax.random.fold_in(jax.random.fold_in(key, 6), position), (shards_of,), jnp.float32, least / len(shards), largest / len(shards))
        return jnp.repeat(jnp.exp(draws), extent[position] // shards_of).reshape((-1,) + (1,) * (len(extent) - position - 1))

    loudness = one(*shards[0])
    for cut in shards[1:]:
        loudness = loudness * one(*cut)
    return loudness


def centred(key, shape, spread, reach, split=(), held_as=jnp.bfloat16):
    array = spread * jax.random.normal(key, shape, jnp.float32)
    if split:
        array = array * shard_levels(key, shape, split, -0.22, 0.18)
    return jnp.clip(array, -reach, reach).astype(held_as)


def heavy_noise(key, dims, width, bound, split, heavy, held_as=jnp.bfloat16):
    result = width * jax.random.normal(key, dims, jnp.float32)
    if split:
        result = result * shard_levels(key, dims, split, -0.22, 0.18)
    return jnp.clip(spiked(result, jax.random.fold_in(key, 3), *heavy), -bound, bound).astype(held_as)


def setup_inputs(seed: int = 0) -> dict:
    arg_keys = jax.random.split(jax.random.key(seed), 16)
    layer_input = heavy_noise(arg_keys[0], (BATCH, LEN, D), 1.0, 6.0, ((0, 16), (1, 16)), (1, 2, 16, 2.0))
    queries = draw_queries(jax.random.fold_in(arg_keys[15], 71), 0)
    key_rows = draw_key_rows(jax.random.fold_in(arg_keys[15], 71), 0)
    value_rows = centred(arg_keys[3], (BATCH, LEN, HH), 1.0, 6.0, ((0, 16), (1, 16)))
    context = centred(arg_keys[4], (BATCH, LEN, HH), 1.0, 6.0, ((0, 16), (1, 16)))
    grad_context = centred(arg_keys[5], (BATCH, LEN, HH), 1.0, 6.0, ((0, 16), (1, 16)))
    grad_output = heavy_noise(arg_keys[6], (BATCH, LEN, D), 1.0, 6.0, ((0, 16), (1, 16)), (1, 2, 16, 2.0))
    earlier_mass = jnp.clip(3.0 + 4.0 * jax.random.uniform(arg_keys[7], (BATCH, H, LEN), jnp.float32) ** shard_levels(arg_keys[7], (BATCH, H, LEN), ((0, 16), (2, 16)), -0.2, 0.2), 3.0, 7.0)
    grad_queries = heavy_noise(arg_keys[8], (BATCH, LEN, HH), 0.02, 0.12, ((0, 16), (1, 16)), (0, 2, 16, 2.0), jnp.float32)
    grad_keys = centred(arg_keys[9], (BATCH, LEN, HH), 0.02, 0.12, ((0, 16), (1, 16)), jnp.float32)
    grad_values = centred(arg_keys[10], (BATCH, LEN, HH), 0.02, 0.12, ((0, 16), (1, 16)), jnp.float32)
    documents = draw_documents(jax.random.fold_in(arg_keys[15], 71), 0)
    weights = centred(arg_keys[12], (4, D, HH), D ** -0.5, 0.125, ((1, 16), (2, 16)), jnp.float32)
    row_factor = jnp.clip(jnp.exp(math.log(1.52587890625e-05) - 6.9077552 * jax.random.uniform(arg_keys[13], (4, D), jnp.float32) ** shard_levels(arg_keys[13], (4, D), ((1, 16),), -0.2, 0.2)), 1.525878978725359e-08, 1.52587890625e-05)
    column_factor = jnp.clip(jnp.exp(math.log(1.52587890625e-05) - 6.9077552 * jax.random.uniform(arg_keys[14], (4, HH), jnp.float32) ** shard_levels(arg_keys[14], (4, HH), ((1, 16),), -0.2, 0.2)), 1.525878978725359e-08, 1.52587890625e-05)
    return {"layer_input": layer_input, "queries": queries, "key_rows": key_rows, "value_rows": value_rows, "context": context, "grad_context": grad_context, "grad_output": grad_output, "earlier_mass": earlier_mass, "grad_queries": grad_queries, "grad_keys": grad_keys, "grad_values": grad_values, "documents": documents, "weights": weights, "row_factor": row_factor, "column_factor": column_factor}


beta_two = 0.9
learn_rate = 0.05
tiny_square = 1e-30
exact = lax.Precision.HIGHEST

def folded_table(blocks, row_count):
    half = row_count // 2
    block_ids = jnp.arange(blocks, dtype=jnp.int32)[:, None]
    local = jnp.arange(row_count, dtype=jnp.int32)[None, :]
    lower = block_ids * half + local
    upper = (2 * blocks - 1 - block_ids) * half + local - half
    return jnp.where(local < half, lower, upper)

def attend_back(queries, key_rows, value_rows, context, grad_context, earlier_mass, allowed):
    row_count = queries.shape[0]
    key_count = key_rows.shape[0]
    head_count = earlier_mass.shape[0]
    head_size = queries.shape[1] // head_count
    scale_factor = 1.0 / math.sqrt(head_size)
    query_heads = queries.astype(jnp.float32).reshape(row_count, head_count, head_size)
    key_heads = key_rows.astype(jnp.float32).reshape(key_count, head_count, head_size)
    value_heads = value_rows.astype(jnp.float32).reshape(key_count, head_count, head_size)
    context_heads = context.astype(jnp.float32).reshape(row_count, head_count, head_size)
    grad_heads = grad_context.astype(jnp.float32).reshape(row_count, head_count, head_size)
    scores = jnp.einsum('thd,shd->hts', query_heads, key_heads, precision=exact) * scale_factor
    open_pairs = allowed[None]
    peak_score = jnp.maximum(earlier_mass, lax.optimization_barrier(jnp.max(jnp.where(open_pairs, scores, -jnp.inf), axis=2)))
    shifted = jnp.where(open_pairs, jnp.exp(scores - peak_score[:, :, None]), 0.0)
    total_mass = jnp.exp(earlier_mass - peak_score) + lax.optimization_barrier(jnp.sum(shifted, axis=2))
    log_norm = peak_score + jnp.log(total_mass)
    attention = jnp.where(open_pairs, jnp.exp(scores - log_norm[:, :, None]), 0.0)
    attention_low = attention.astype(jnp.bfloat16).astype(jnp.float32)
    row_dot = lax.optimization_barrier(jnp.sum(context_heads * grad_heads, axis=2)).T
    grad_attention = jnp.einsum('thd,shd->hts', grad_heads, value_heads, precision=exact)
    grad_scores = (attention * (grad_attention - row_dot[:, :, None]) * scale_factor).astype(jnp.bfloat16).astype(jnp.float32)
    query_step = jnp.einsum('hts,shd->thd', grad_scores, key_heads, precision=exact).reshape(row_count, -1)
    key_step = jnp.einsum('hts,thd->shd', grad_scores, query_heads, precision=exact).reshape(key_count, -1)
    value_step = jnp.einsum('hts,thd->shd', attention_low, grad_heads, precision=exact).reshape(key_count, -1)
    return (query_step, key_step, value_step)

def reference(layer_input, queries, key_rows, value_rows, context, grad_context, grad_output, earlier_mass, grad_queries, grad_keys, grad_values, documents, weights, row_factor, column_factor):
    blocks = N_BLK
    row_count = TOK_DEV
    positions = folded_table(blocks, row_count)
    seen_pos = jnp.concatenate([jnp.roll(positions, -1, axis=0), jnp.roll(positions, -2, axis=0)], axis=1)
    causal = seen_pos[:, None, :] <= positions[:, :, None]

    def visited(blocked):
        return jnp.concatenate([jnp.roll(blocked, -1, axis=0), jnp.roll(blocked, -2, axis=0)], axis=1)

    def one_sequence(items):
        query_seq, key_seq, value_seq, context_seq, grad_seq, mass_seq, doc_seq = items
        query_blocks = query_seq.reshape(blocks, row_count, -1)
        key_seen = visited(key_seq.reshape(blocks, row_count, -1))
        value_seen = visited(value_seq.reshape(blocks, row_count, -1))
        context_blocks = context_seq.reshape(blocks, row_count, -1)
        grad_blocks = grad_seq.reshape(blocks, row_count, -1)
        doc_blocks = doc_seq.reshape(blocks, row_count)
        doc_seen = visited(doc_blocks)
        allowed = causal & (doc_seen[:, None, :] == doc_blocks[:, :, None])
        mass_blocks = jnp.transpose(mass_seq.reshape(mass_seq.shape[0], blocks, row_count), (1, 0, 2))
        query_step, key_step, value_step = jax.vmap(attend_back)(query_blocks, key_seen, value_seen, context_blocks, grad_blocks, mass_blocks, allowed)
        key_home = jnp.roll(key_step[:, :row_count], 1, axis=0) + jnp.roll(key_step[:, row_count:], 2, axis=0)
        value_home = jnp.roll(value_step[:, :row_count], 1, axis=0) + jnp.roll(value_step[:, row_count:], 2, axis=0)
        return (query_step.reshape(LEN, -1), key_home.reshape(LEN, -1), value_home.reshape(LEN, -1))
    query_add, key_add, value_add = lax.map(one_sequence, (queries, key_rows, value_rows, context, grad_context, earlier_mass, documents))
    query_total = grad_queries + query_add
    key_total = grad_keys + key_add
    value_total = grad_values + value_add
    units = BATCH * blocks
    right_low = jnp.stack([query_total, key_total, value_total], axis=2).astype(jnp.bfloat16).reshape(units, row_count, 3, HH)
    left_units = layer_input.reshape(units, row_count, D)
    outer_units = grad_output.reshape(units, row_count, D)
    inner_units = context.reshape(units, row_count, HH)

    def add_unit(total, unit):
        left_part, right_part, outer_part, inner_part = unit
        part_inner = jnp.einsum('td,twh->dwh', left_part.astype(jnp.float32), right_part.astype(jnp.float32), precision=exact)
        part_output = jnp.einsum('td,th->dh', outer_part.astype(jnp.float32), inner_part.astype(jnp.float32), precision=exact)
        partial_value = jnp.concatenate([part_inner, part_output[:, None, :]], axis=1)
        rounded = lax.optimization_barrier(partial_value.astype(jnp.bfloat16))
        return (total + rounded.astype(jnp.float32), None)
    total, unused = lax.scan(add_unit, jnp.zeros((D, 4, HH), jnp.float32), (left_units, right_low, outer_units, inner_units))
    gradient = jnp.transpose(total, (1, 0, 2)) / (BATCH * LEN)
    squares = gradient * gradient + tiny_square
    new_row_factor = beta_two * row_factor + (1.0 - beta_two) * lax.optimization_barrier(jnp.mean(squares, axis=2))
    new_column_factor = beta_two * column_factor + (1.0 - beta_two) * lax.optimization_barrier(jnp.mean(squares, axis=1))
    row_mean = lax.optimization_barrier(jnp.mean(new_row_factor, axis=1))
    second = new_row_factor[:, :, None] * new_column_factor[:, None, :] / row_mean[:, None, None]
    new_weights = weights - learn_rate * gradient * lax.rsqrt(second)
    return (new_weights, new_row_factor, new_column_factor)
```

```python
from types import SimpleNamespace

import jax
import jax.numpy as jnp
from jax import lax
from jax.experimental import pallas as pl
from jax.experimental.pallas import tpu as pltpu
from jax.sharding import PartitionSpec as P

beta_two = 0.9
learn_rate = 0.05
tiny_square = 1e-30
low = jnp.bfloat16
full = jnp.float32
ALL_TOKENS = 65536.0
SCALE = 1.0 / 16.0

NT = (((1,), (1,)), ((), ()))
NN = (((1,), (0,)), ((), ()))
TN = (((0,), (0,)), ((), ()))


def dot(a, b, dims):
    return lax.dot_general(a, b, dims, preferred_element_type=full)


def group_scratch(tag, w):
    return {
        "p_" + tag: pltpu.VMEM((4, 2, 4, w, 64, 512), low),
        "xa_" + tag: pltpu.VMEM((2, 2, w, 64, 512), low),
        "xb_" + tag: pltpu.VMEM((2, 4, w, 64, 512), low),
        "ya_" + tag: pltpu.VMEM((2, w, 32, 512), low),
        "yb_" + tag: pltpu.VMEM((2, w, 64, 512), low),
        "ea_" + tag: pltpu.VMEM((4, 2, w, 32, 512), low),
        "eb_" + tag: pltpu.VMEM((4, 2, w, 64, 512), low),
        "fa_" + tag: pltpu.VMEM((2, w, 32, 512), low),
        "fb_" + tag: pltpu.VMEM((2, w, 64, 512), low),
        "zs_" + tag: pltpu.VMEM((8, w, 64, 128), low),
        "zr_" + tag: pltpu.VMEM((8, w, 64, 128), low),
        "rtf_" + tag: pltpu.VMEM((4, w, 2, 2, 64, 256), low),
        "rtp_" + tag: pltpu.VMEM((4, w, 2, 64, 256), low),
    }


N_SEM = 160
SCRATCH = {
    "ly": pltpu.VMEM((2, 256, 2048), low),
    "gt": pltpu.VMEM((2, 256, 2048), low),
    "cx": pltpu.VMEM((4, 256, 256), low),
    "gox": pltpu.VMEM((4, 256, 256), low),
    "kk": pltpu.VMEM((4, 512, 256), low),
    "vv": pltpu.VMEM((4, 512, 256), low),
    "qr": pltpu.VMEM((4, 2, 128, 256), low),
    "orr": pltpu.VMEM((4, 2, 128, 256), low),
    "gqs": pltpu.VMEM((4, 256, 256), full),
    "gks": pltpu.VMEM((4, 256, 256), full),
    "gvs": pltpu.VMEM((4, 256, 256), full),
    "meta": pltpu.VMEM((4, 8, 256), full),
    "mr": pltpu.VMEM((4, 8, 256), full),
    "ds": pltpu.VMEM((8, 256), full),
    "dr": pltpu.VMEM((8, 256), full),
    "dk": pltpu.VMEM((512, 128), full),
    "acck": pltpu.VMEM((256, 256), full),
    "accv": pltpu.VMEM((256, 256), full),
    "dqs": pltpu.VMEM((4, 2, 128, 256), low),
    "dks": pltpu.VMEM((4, 256, 256), low),
    "dvs": pltpu.VMEM((4, 256, 256), low),
    "dqr": pltpu.VMEM((4, 2, 128, 256), low),
    "dkr": pltpu.VMEM((4, 256, 256), low),
    "dvr": pltpu.VMEM((4, 256, 256), low),
    "rows": pltpu.VMEM((8, 128), full),
    "cols": pltpu.VMEM((8, 128), full),
    "tot": pltpu.VMEM((8, 128), full),
    "rowr": pltpu.VMEM((16, 8, 128), full),
    "colr": pltpu.VMEM((16, 8, 128), full),
    "totr": pltpu.VMEM((16, 8, 128), full),
    "grad": pltpu.VMEM((4, 64, 128), full),
    **group_scratch("o", 1),
    **group_scratch("m", 3),
    "send": pltpu.SemaphoreType.DMA((N_SEM,)),
    "recv": pltpu.SemaphoreType.DMA((N_SEM,)),
    "local": pltpu.SemaphoreType.DMA((40,)),
    "stat_send": pltpu.SemaphoreType.DMA((3, 16)),
    "stat_recv": pltpu.SemaphoreType.DMA((3, 16)),
}


def kernel(lay, q, k, v, ctx, go, gout, mass, gq, gk, gv, docs, wts, rf, cf, ow, orf, ocf, *scr):
    s = SimpleNamespace(**dict(zip(SCRATCH, scr)))
    dp = lax.axis_index("dp")
    b = lax.axis_index("blk")
    x = lax.div(dp, 4)
    yl = lax.rem(lax.div(dp, 2), 2)
    c = lax.rem(dp, 2)
    yh = lax.div(b, 8)
    z = lax.rem(b, 8)
    y = yh * 2 + yl

    def at(x_, y_, z_):
        return {"dp": x_ * 4 + lax.rem(y_, 2) * 2 + c, "blk": lax.div(y_, 2) * 8 + z_}

    up_x, dn_x = at(lax.rem(x + 1, 4), y, z), at(lax.rem(x + 3, 4), y, z)
    up_y, dn_y = at(x, lax.rem(y + 1, 4), z), at(x, lax.rem(y + 3, 4), z)
    y_one, y_two, y_three = lax.rem(y + 1, 4), lax.rem(y + 2, 4), lax.rem(y + 3, 4)
    mate = {"dp": dp + 1 - 2 * c, "blk": b}
    up_b, dn_b = {"dp": dp, "blk": lax.rem(b + 1, 16)}, {"dp": dp, "blk": lax.rem(b + 15, 16)}
    heads = [lax.rem(x + 2, 4), lax.rem(x + 1, 4), lax.rem(x + 3, 4), x]
    cols = [pl.ds(pl.multiple_of(h * 256, 256), 256) for h in heads]

    barrier = pltpu.get_barrier_semaphore()

    def greet(p, carry):
        pl.semaphore_signal(
            barrier, inc=1, device_id={"dp": lax.rem(dp + p, 16), "blk": b},
            device_id_type=pl.DeviceIdType.MESH,
        )
        pl.semaphore_signal(
            barrier, inc=1, device_id={"dp": dp, "blk": lax.rem(b + p, 16)},
            device_id_type=pl.DeviceIdType.MESH,
        )
        return carry

    lax.fori_loop(1, 16, greet, 0)
    pl.semaphore_signal(
        barrier, inc=1, device_id=at(x, 3 - y, z), device_id_type=pl.DeviceIdType.MESH
    )

    used = [0, 0]
    to_finish = []

    def local(src, dst):
        copy = pltpu.make_async_copy(src, dst, s.local.at[used[1]])
        used[1] += 1
        copy.start()
        return copy

    def remote(src, dst, device, cond=None):
        n = used[0]
        used[0] += 1
        copy = pltpu.make_async_remote_copy(
            src_ref=src, dst_ref=dst, send_sem=s.send.at[n], recv_sem=s.recv.at[n],
            device_id=device, device_id_type=pl.DeviceIdType.MESH,
        )
        if cond is None:
            copy.start()
        else:
            @pl.when(cond)
            def _():
                copy.start()
        to_finish.append((copy, cond))
        return copy

    def arrived(copy, cond=None):
        if cond is None:
            copy.wait_recv()
        else:
            @pl.when(cond)
            def _():
                copy.wait_recv()

    wrapped = (b == 0) | (b == 15)
    sends_low_q = b >= 14
    sends_up_k = b >= 2
    plain = (b >= 1) & (b <= 14)

    load_cx = [local(ctx.at[:, cols[i]], s.cx.at[i]) for i in range(4)]
    load_go = [local(go.at[:, cols[i]], s.gox.at[i]) for i in range(4)]
    load_kv = []
    for i in range(4):
        load_kv.append(
            (
                local(k.at[:, cols[i]], s.kk.at[i, pl.ds(0, 256)]),
                local(v.at[:, cols[i]], s.vv.at[i, pl.ds(0, 256)]),
            )
        )
    load_gt = local(gout, s.gt.at[0])
    load_ly = local(lay, s.ly.at[0])
    load_g = []
    for i in range(4):
        load_g.append(
            (
                local(gq.at[:, cols[i]], s.gqs.at[i]),
                local(gk.at[:, cols[i]], s.gks.at[i]),
                local(gv.at[:, cols[i]], s.gvs.at[i]),
            )
        )

    own_docs = docs[...].astype(full)
    s.ds[...] = jnp.broadcast_to(own_docs, (8, 256))
    s.dk[pl.ds(0, 256), :] = jnp.transpose(jnp.broadcast_to(own_docs, (128, 256)))
    ones = jnp.ones((8, 256), low)
    for i in range(4):
        load_cx[i].wait()
        load_go[i].wait()
        product = s.cx[i].astype(full) * s.gox[i].astype(full)
        high_part = product.astype(low)
        low_part = (product - high_part.astype(full)).astype(low)
        row_dot = dot(ones, high_part, NT) + dot(ones, low_part, NT)
        s.meta[i, pl.ds(0, 1), :] = mass[pl.ds(heads[i], 1), :]
        s.meta[i, pl.ds(1, 1), :] = row_dot[0:1, :]
        s.meta[i, pl.ds(2, 1), :] = own_docs
        s.rtf_o[i, 0] = jnp.transpose(s.cx[i]).reshape(2, 2, 64, 256)

    @pl.when(wrapped)
    def _():
        for i in range(4):
            s.kk[i, pl.ds(384, 128), :] = jnp.zeros((128, 256), low)
            s.vv[i, pl.ds(384, 128), :] = jnp.zeros((128, 256), low)

    pl.semaphore_wait(barrier, 31)

    lower, upper = pl.ds(0, 128), pl.ds(128, 128)
    go_meta = remote(s.meta, s.mr, up_b)
    go_docs = remote(s.ds, s.dr, dn_b)
    send_rto = remote(s.rtf_o.at[:, :, :, 1 - c], s.rtp_o, mate)
    send_gt = remote(gout, s.gt.at[1], mate)
    forward = []
    for i in range(4):
        forward.append(
            [
                (remote(k.at[lower, cols[i]], s.kk.at[i, pl.ds(256, 128)], dn_b), None),
                (remote(q.at[upper, cols[i]], s.qr.at[i, 0], up_b), None),
                (remote(k.at[upper, cols[i]], s.kk.at[i, pl.ds(384, 128)], dn_b, sends_up_k), plain),
                (remote(q.at[lower, cols[i]], s.qr.at[i, 1], up_b, sends_low_q), wrapped),
                (remote(v.at[lower, cols[i]], s.vv.at[i, pl.ds(256, 128)], dn_b), None),
                (remote(go.at[upper, cols[i]], s.orr.at[i, 0], up_b), None),
                (remote(v.at[upper, cols[i]], s.vv.at[i, pl.ds(384, 128)], dn_b, sends_up_k), plain),
                (remote(go.at[lower, cols[i]], s.orr.at[i, 1], up_b, sends_low_q), wrapped),
            ]
        )
    send_ly = remote(lay, s.ly.at[1], mate)

    def weight_part(left, mate_left, right, p_ref, i, w):
        def block(db, carry):
            lanes = pl.ds(pl.multiple_of(db * 256, 256), 256)
            out = dot(left, right[0, :, lanes], NN) + dot(mate_left, right[1, :, lanes], NN)
            out = out.astype(low).reshape(-1, w, 2, 64, 256)
            y_hi = lax.div(db, 4)
            half = lax.rem(lax.div(db, 2), 2)
            at_lane = pl.ds(pl.multiple_of(lax.rem(db, 2) * 256, 256), 256)
            for n in range(out.shape[0]):
                for one in range(2):
                    p_ref[i + n, half, y_hi * 2 + one, :, :, at_lane] = out[n, :, one]
            return carry

        lax.fori_loop(0, 8, block, 0)

    def add_to(ref, *others):
        total = ref[...].astype(full)
        for other in others:
            total = total + other[...].astype(full)
        ref[...] = total.astype(low)

    top, bottom = pl.ds(0, 32), pl.ds(32, 32)

    class Group:
        def __init__(self, tag, w):
            self.w = w
            for name in ("p", "xa", "xb", "ya", "yb", "ea", "eb", "fa", "fb", "zs", "zr", "rtf", "rtp"):
                setattr(self, name, getattr(s, name + "_" + tag))
            self.ea_copy, self.eb_copy = {}, {}

        def x_first(self, i):
            p = self.p
            if i == 0:
                self.xa0 = remote(p.at[0, 0, pl.ds(0, 2)], self.xa.at[0], up_x)
                self.xa1 = remote(p.at[0, 0, pl.ds(2, 2)], self.xa.at[1], dn_x)
            elif i == 1:
                arrived(self.xa0)
                add_to(p.at[1, 0, pl.ds(0, 2)], self.xa.at[0])
                self.xb0 = remote(p.at[1, 0], self.xb.at[0], up_x)
            elif i == 2:
                arrived(self.xa1)
                add_to(p.at[2, 0, pl.ds(2, 2)], self.xa.at[1])
                self.xb1 = remote(p.at[2, 0], self.xb.at[1], dn_x)

        def x_first_end(self):
            p = self.p
            arrived(self.xb0)
            arrived(self.xb1)
            add_to(p.at[3, 0], self.xb.at[0], self.xb.at[1])
            self.ya0 = remote(p.at[3, 0, y_two, :, top], self.ya.at[0], up_y)
            self.ya1 = remote(p.at[3, 0, y_two, :, bottom], self.ya.at[1], dn_y)

        def then_y(self):
            p = self.p
            arrived(self.ya0)
            add_to(p.at[3, 0, y_one, :, top], self.ya.at[0])
            self.yb0 = remote(p.at[3, 0, y_one], self.yb.at[0], up_y)
            arrived(self.ya1)
            add_to(p.at[3, 0, y_three, :, bottom], self.ya.at[1])
            self.yb1 = remote(p.at[3, 0, y_three], self.yb.at[1], dn_y)

        def y_first(self, i):
            p = self.p
            self.ea_copy[i] = (
                remote(p.at[i, 1, y_two, :, top], self.ea.at[i, 0], up_y),
                remote(p.at[i, 1, y_two, :, bottom], self.ea.at[i, 1], dn_y),
            )

        def y_second(self, i):
            p = self.p
            arrived(self.ea_copy[i][0])
            add_to(p.at[i, 1, y_one, :, top], self.ea.at[i, 0])
            first = remote(p.at[i, 1, y_one], self.eb.at[i, 0], up_y)
            arrived(self.ea_copy[i][1])
            add_to(p.at[i, 1, y_three, :, bottom], self.ea.at[i, 1])
            self.eb_copy[i] = (first, remote(p.at[i, 1, y_three], self.eb.at[i, 1], dn_y))

        def y_end_then_x(self, i):
            p = self.p
            arrived(self.eb_copy[i][0])
            arrived(self.eb_copy[i][1])
            mine = p.at[i, 1, y]
            add_to(mine, self.eb.at[i, 0], self.eb.at[i, 1])
            if i == 0:
                self.fa0 = remote(p.at[0, 1, y, :, top], self.fa.at[0], up_x)
                self.fa1 = remote(p.at[0, 1, y, :, bottom], self.fa.at[1], dn_x)
            elif i == 1:
                arrived(self.fa0)
                add_to(p.at[1, 1, y, :, top], self.fa.at[0])
                self.fb0 = remote(mine, self.fb.at[0], up_x)
            elif i == 2:
                arrived(self.fa1)
                add_to(p.at[2, 1, y, :, bottom], self.fa.at[1])
                self.fb1 = remote(mine, self.fb.at[1], dn_x)

        def stage(self, mine, one, two, base):
            total = mine[...].astype(full) + one[...].astype(full) + two[...].astype(full)
            total = total.astype(low)
            for n in range(4):
                self.zs[base + n] = total[:, :, n * 128 : (n + 1) * 128]

        def along_z(self):
            arrived(self.yb0)
            arrived(self.yb1)
            self.stage(self.p.at[3, 0, y], self.yb.at[0], self.yb.at[1], 0)
            arrived(self.fb0)
            arrived(self.fb1)
            self.stage(self.p.at[3, 1, y], self.fb.at[0], self.fb.at[1], 4)
            self.z_copies = []
            for p in (4, 3, 5, 2, 6, 1, 7):
                there = lax.rem(z + p, 8)
                self.z_copies.append(remote(self.zs.at[there], self.zr.at[p], at(x, y, there)))

        def total(self):
            for copy in self.z_copies:
                arrived(copy)
            total = self.zs[z].astype(full)
            for p in range(1, 8):
                total = total + self.zr[p].astype(full)
            return total

    out_g, main_g = Group("o", 1), Group("m", 3)

    load_gt.wait()
    arrived(send_rto)
    arrived(send_gt)
    weight_part(
        s.rtf_o[:, :, :, c].reshape(512, 256), s.rtp_o[...].reshape(512, 256), s.gt, s.p_o, 0, 1
    )
    out_g.x_first(0)
    for i in range(4):
        out_g.y_first(i)

    j = lax.rem(b + 15, 16)
    halves_here = jnp.where(wrapped, 2, 1)
    row = lax.broadcasted_iota(jnp.int32, (512, 128), 0)
    key_block = jnp.where(row < 256, b, lax.rem(b + 1, 16))
    key_low = (row < 128) | ((row >= 256) & (row < 384))
    key_place = jnp.where(key_low, key_block, 31 - key_block)

    returns = {}

    def attention(i):
        for copy, cond in forward[i]:
            arrived(copy, cond)
        for copy in load_kv[i] + load_g[i]:
            copy.wait()
        s.acck[...] = jnp.zeros((256, 256), full)
        s.accv[...] = jnp.zeros((256, 256), full)

        def one_half(r, carry):
            lanes = pl.ds(pl.multiple_of((1 - r) * 128, 128), 128)
            query = s.qr[i, r]
            grad = s.orr[i, r]
            mass_row = s.mr[i, pl.ds(0, 1), lanes]
            dot_row = s.mr[i, pl.ds(1, 1), lanes]
            docs_row = s.mr[i, pl.ds(2, 1), lanes]
            place = jnp.where(r == 0, 31 - j, j)
            open_pairs = (s.dk[...] == docs_row) & (key_place < place)
            keys = s.kk[i]
            scores = dot(keys, query, NT) * SCALE
            scores = jnp.where(open_pairs, scores, -jnp.inf)
            peak = jnp.maximum(mass_row, jnp.max(scores, axis=0, keepdims=True))
            shifted = jnp.exp(scores - peak)
            norm = jnp.exp(mass_row - peak) + jnp.sum(shifted, axis=0, keepdims=True)
            attention_part = shifted * (1.0 / norm)
            grad_attention = dot(s.vv[i], grad, NT)
            grad_scores = (attention_part * (grad_attention - dot_row) * SCALE).astype(low)
            value_step = dot(attention_part.astype(low), grad, NN)
            key_step = dot(grad_scores, query, NN)
            s.gks[i] += key_step[0:256]
            s.gvs[i] += value_step[0:256]
            s.acck[...] += key_step[256:512]
            s.accv[...] += value_step[256:512]
            s.dqs[i, r] = dot(jnp.transpose(grad_scores), keys, NN).astype(low)
            return carry

        lax.fori_loop(0, halves_here, one_half, 0)
        s.dks[i] = s.acck[...].astype(low)
        s.dvs[i] = s.accv[...].astype(low)
        returns[i] = [
            (remote(s.dqs.at[i, 0], s.dqr.at[i, 0], dn_b), None),
            (remote(s.dqs.at[i, 1], s.dqr.at[i, 1], dn_b, wrapped), sends_low_q),
            (remote(s.dks.at[i, lower], s.dkr.at[i, lower], up_b), None),
            (remote(s.dks.at[i, upper], s.dkr.at[i, upper], up_b, plain), sends_up_k),
            (remote(s.dvs.at[i, lower], s.dvr.at[i, lower], up_b), None),
            (remote(s.dvs.at[i, upper], s.dvr.at[i, upper], up_b, plain), sends_up_k),
        ]

    exchanged = {}

    def finalize(i):
        for copy, cond in returns[i]:
            arrived(copy, cond)
        s.gqs[i, upper, :] += s.dqr[i, 0].astype(full)
        s.gks[i, lower, :] += s.dkr[i, lower, :].astype(full)
        s.gvs[i, lower, :] += s.dvr[i, lower, :].astype(full)

        @pl.when(sends_low_q)
        def _():
            s.gqs[i, lower, :] += s.dqr[i, 1].astype(full)

        @pl.when(sends_up_k)
        def _():
            s.gks[i, upper, :] += s.dkr[i, upper, :].astype(full)
            s.gvs[i, upper, :] += s.dvr[i, upper, :].astype(full)

        for w, total in enumerate((s.gqs, s.gks, s.gvs)):
            s.rtf_m[i, w] = jnp.transpose(total[i].astype(low)).reshape(2, 2, 64, 256)
        exchanged[i] = remote(s.rtf_m.at[i, :, :, 1 - c], s.rtp_m.at[i], mate)

    def weights_of(i):
        arrived(exchanged[i])
        weight_part(
            s.rtf_m[i, :, :, c].reshape(384, 256), s.rtp_m[i].reshape(384, 256), s.ly, s.p_m, i, 3
        )
        main_g.x_first(i)
        main_g.y_first(i)

    arrived(go_meta)
    arrived(go_docs)
    s.dk[pl.ds(256, 256), :] = jnp.transpose(jnp.broadcast_to(s.dr[0:1, :], (128, 256)))
    attention(0)
    out_g.x_first(1)
    out_g.x_first(2)
    for i in range(4):
        out_g.y_second(i)
    attention(1)
    finalize(0)
    for i in range(3):
        out_g.y_end_then_x(i)
    out_g.x_first_end()
    load_ly.wait()
    arrived(send_ly)
    weights_of(0)
    attention(2)
    finalize(1)
    main_g.y_second(0)
    weights_of(1)
    out_g.y_end_then_x(3)
    out_g.then_y()
    attention(3)
    finalize(2)
    main_g.y_end_then_x(0)
    main_g.y_second(1)
    weights_of(2)
    out_g.along_z()
    finalize(3)
    main_g.y_end_then_x(1)
    main_g.y_second(2)
    weights_of(3)
    main_g.y_end_then_x(2)
    main_g.x_first_end()
    main_g.y_second(3)
    main_g.then_y()
    main_g.y_end_then_x(3)
    main_g.along_z()
    s.grad[3] = out_g.total()[0] * (1.0 / ALL_TOKENS)
    s.grad[pl.ds(0, 3)] = main_g.total() * (1.0 / ALL_TOKENS)

    s.rows[...] = jnp.zeros((8, 128), full)
    s.cols[...] = jnp.zeros((8, 128), full)
    for w in range(4):
        squares = s.grad[w] * s.grad[w] + tiny_square
        s.rows[pl.ds(w, 1), :] = jnp.sum(squares, axis=0, keepdims=True)
        s.cols[pl.ds(w, 1), pl.ds(0, 64)] = jnp.sum(jnp.transpose(squares), axis=0, keepdims=True)
    s.rowr[pl.ds(0, 1)] = s.rows[...][None]
    s.colr[pl.ds(0, 1)] = s.cols[...][None]

    def stat_copy(src, dst, n, p, device):
        return pltpu.make_async_remote_copy(
            src_ref=src, dst_ref=dst, send_sem=s.stat_send.at[n, p], recv_sem=s.stat_recv.at[n, p],
            device_id=device, device_id_type=pl.DeviceIdType.MESH,
        )

    def row_copy(p):
        return stat_copy(s.rows, s.rowr.at[p], 0, p, {"dp": lax.rem(dp + p, 16), "blk": b})

    def col_copy(p):
        return stat_copy(s.cols, s.colr.at[p], 1, p, {"dp": dp, "blk": lax.rem(b + p, 16)})

    def tot_copy(p):
        return stat_copy(s.tot, s.totr.at[p], 2, p, {"dp": dp, "blk": lax.rem(b + p, 16)})

    def each(action):
        def step(p, carry):
            action(p)
            return carry

        lax.fori_loop(1, 16, step, 0)

    each(lambda p: row_copy(p).start())
    each(lambda p: col_copy(p).start())
    each(lambda p: row_copy(p).wait_recv())
    row_sum = jnp.sum(s.rowr[...], axis=0)[0:4]
    new_row = beta_two * rf[...] + (1.0 - beta_two) * (row_sum / 1024.0)
    orf[...] = new_row
    s.tot[...] = jnp.zeros((8, 128), full)
    s.tot[pl.ds(0, 4), :] = new_row
    s.totr[pl.ds(0, 1)] = s.tot[...][None]
    each(lambda p: tot_copy(p).start())
    each(lambda p: col_copy(p).wait_recv())
    col_sum = jnp.sum(s.colr[...], axis=0)[0:4, 0:64]
    new_col = beta_two * cf[...] + (1.0 - beta_two) * (col_sum / 2048.0)
    ocf[...] = new_col
    each(lambda p: tot_copy(p).wait_recv())
    all_rows = jnp.sum(s.totr[...], axis=0)[0:4]
    row_mean = jnp.sum(all_rows, axis=1, keepdims=True) / 2048.0
    for w in range(4):
        col_wide = jnp.transpose(jnp.broadcast_to(new_col[w : w + 1, :], (128, 64)))
        second = new_row[w : w + 1, :] * col_wide / row_mean[w : w + 1, :]
        update = learn_rate * s.grad[w] * lax.rsqrt(second)
        ow[w] = wts[w] - jnp.transpose(update)

    each(lambda p: row_copy(p).wait_send())
    each(lambda p: col_copy(p).wait_send())
    each(lambda p: tot_copy(p).wait_send())
    for copy, cond in to_finish:
        if cond is None:
            copy.wait_send()
        else:
            @pl.when(cond)
            def _(copy=copy):
                copy.wait_send()


def body(
    layer_input, queries, key_rows, value_rows, context, grad_context, grad_output, earlier_mass,
    grad_queries, grad_keys, grad_values, documents, weights, row_factor, column_factor,
):
    far = pl.BlockSpec(memory_space=pl.ANY)
    near = pl.BlockSpec(memory_space=pltpu.VMEM)
    return pl.pallas_call(
        kernel,
        out_shape=(
            jax.ShapeDtypeStruct((4, 128, 64), full),
            jax.ShapeDtypeStruct((4, 128), full),
            jax.ShapeDtypeStruct((4, 64), full),
        ),
        in_specs=[far] * 7 + [near] + [far] * 3 + [near] * 4,
        out_specs=(near, near, near),
        scratch_shapes=list(SCRATCH.values()),
        compiler_params=pltpu.CompilerParams(
            collective_id=0, has_side_effects=True, vmem_limit_bytes=60 * 1024 * 1024
        ),
    )(
        layer_input[0], queries[0], key_rows[0], value_rows[0], context[0], grad_context[0],
        grad_output[0], earlier_mass[0], grad_queries[0], grad_keys[0], grad_values[0], documents,
        weights, row_factor, column_factor,
    )


def solution(mesh):
    placed = (P("dp", "blk", None),) * 7 + (P("dp", None, "blk"),) + (P("dp", "blk", None),) * 3 + (
        P("dp", "blk"),
        P(None, "blk", "dp"),
        P(None, "blk"),
        P(None, "dp"),
    )
    return jax.shard_map(
        body,
        mesh=mesh,
        in_specs=placed,
        out_specs=(P(None, "blk", "dp"), P(None, "blk"), P(None, "dp")),
        check_vma=False,
    )
```

```python
from types import SimpleNamespace

import jax
import jax.numpy as jnp
from jax import lax
from jax.experimental import pallas as pl
from jax.experimental.pallas import tpu as pltpu
from jax.sharding import PartitionSpec as P

beta_two = 0.9
learn_rate = 0.05
tiny_square = 1e-30
low = jnp.bfloat16
full = jnp.float32
ALL_TOKENS = 65536.0
SCALE = 1.0 / 16.0

NT = (((1,), (1,)), ((), ()))
NN = (((1,), (0,)), ((), ()))
TN = (((0,), (0,)), ((), ()))


def dot(a, b, dims):
    return lax.dot_general(a, b, dims, preferred_element_type=full)


def group_scratch(tag, w, lanes):
    return {
        "p_" + tag: pltpu.VMEM((4, 1024 // lanes, 4, w, 64, lanes), low),
        "xa_" + tag: pltpu.VMEM((2, 2, w, 64, lanes), low),
        "xb_" + tag: pltpu.VMEM((2, 4, w, 64, lanes), low),
        "ya_" + tag: pltpu.VMEM((2, w, 32, lanes), low),
        "yb_" + tag: pltpu.VMEM((2, w, 64, lanes), low),
        "ea_" + tag: pltpu.VMEM((4, 2, w, 32, 512), low),
        "eb_" + tag: pltpu.VMEM((4, 2, w, 64, 512), low),
        "fa_" + tag: pltpu.VMEM((2, w, 32, 512), low),
        "fb_" + tag: pltpu.VMEM((2, w, 64, 512), low),
        "zs_" + tag: pltpu.VMEM((8, w, 64, 128), low),
        "zr_" + tag: pltpu.VMEM((8, w, 64, 128), low),
        "rtf_" + tag: pltpu.VMEM((4, w, 2, 2, 64, 256), low),
        "rtp_" + tag: pltpu.VMEM((4, w, 2, 64, 256), low),
    }


N_SEM = 240
SCRATCH = {
    "ly": pltpu.VMEM((2, 256, 2048), low),
    "gt": pltpu.VMEM((2, 256, 2048), low),
    "cx": pltpu.VMEM((4, 256, 256), low),
    "gox": pltpu.VMEM((4, 256, 256), low),
    "kk": pltpu.VMEM((4, 512, 256), low),
    "vv": pltpu.VMEM((4, 512, 256), low),
    "qr": pltpu.VMEM((4, 2, 128, 256), low),
    "orr": pltpu.VMEM((4, 2, 128, 256), low),
    "gqs": pltpu.VMEM((4, 256, 256), full),
    "gks": pltpu.VMEM((4, 256, 256), full),
    "gvs": pltpu.VMEM((4, 256, 256), full),
    "meta": pltpu.VMEM((4, 8, 256), full),
    "mr": pltpu.VMEM((4, 8, 256), full),
    "ds": pltpu.VMEM((8, 256), full),
    "dr": pltpu.VMEM((8, 256), full),
    "dk": pltpu.VMEM((512, 128), full),
    "acck": pltpu.VMEM((256, 256), full),
    "accv": pltpu.VMEM((256, 256), full),
    "dqs": pltpu.VMEM((4, 2, 128, 256), low),
    "dks": pltpu.VMEM((4, 256, 256), low),
    "dvs": pltpu.VMEM((4, 256, 256), low),
    "dqr": pltpu.VMEM((4, 2, 128, 256), low),
    "dkr": pltpu.VMEM((4, 256, 256), low),
    "dvr": pltpu.VMEM((4, 256, 256), low),
    "rows": pltpu.VMEM((8, 128), full),
    "cols": pltpu.VMEM((8, 128), full),
    "tot": pltpu.VMEM((8, 128), full),
    "rowr": pltpu.VMEM((16, 8, 128), full),
    "colr": pltpu.VMEM((16, 8, 128), full),
    "totr": pltpu.VMEM((16, 8, 128), full),
    "grad": pltpu.VMEM((4, 64, 128), full),
    "z_send": pltpu.SemaphoreType.DMA((2, 8)),
    "z_recv": pltpu.SemaphoreType.DMA((2, 8)),
    **group_scratch("o", 1, 1024),
    **group_scratch("m", 3, 512),
    "send": pltpu.SemaphoreType.DMA((N_SEM,)),
    "recv": pltpu.SemaphoreType.DMA((N_SEM,)),
    "local": pltpu.SemaphoreType.DMA((40,)),
    "stat_send": pltpu.SemaphoreType.DMA((3, 16)),
    "stat_recv": pltpu.SemaphoreType.DMA((3, 16)),
}


def kernel(lay, q, k, v, ctx, go, gout, mass, gq, gk, gv, docs, wts, rf, cf, ow, orf, ocf, *scr):
    s = SimpleNamespace(**dict(zip(SCRATCH, scr)))
    dp = lax.axis_index("dp")
    b = lax.axis_index("blk")
    x = lax.div(dp, 4)
    yl = lax.rem(lax.div(dp, 2), 2)
    c = lax.rem(dp, 2)
    yh = lax.div(b, 8)
    z = lax.rem(b, 8)
    y = yh * 2 + yl

    def at(x_, y_, z_):
        return {"dp": x_ * 4 + lax.rem(y_, 2) * 2 + c, "blk": lax.div(y_, 2) * 8 + z_}

    up_x, dn_x = at(lax.rem(x + 1, 4), y, z), at(lax.rem(x + 3, 4), y, z)
    up_y, dn_y = at(x, lax.rem(y + 1, 4), z), at(x, lax.rem(y + 3, 4), z)
    y_one, y_two, y_three = lax.rem(y + 1, 4), lax.rem(y + 2, 4), lax.rem(y + 3, 4)
    mate = {"dp": dp + 1 - 2 * c, "blk": b}
    up_b, dn_b = {"dp": dp, "blk": lax.rem(b + 1, 16)}, {"dp": dp, "blk": lax.rem(b + 15, 16)}
    heads = [lax.rem(x + 2, 4), lax.rem(x + 1, 4), lax.rem(x + 3, 4), x]
    cols = [pl.ds(pl.multiple_of(h * 256, 256), 256) for h in heads]

    barrier = pltpu.get_barrier_semaphore()

    def greet(p, carry):
        pl.semaphore_signal(
            barrier, inc=1, device_id={"dp": lax.rem(dp + p, 16), "blk": b},
            device_id_type=pl.DeviceIdType.MESH,
        )
        pl.semaphore_signal(
            barrier, inc=1, device_id={"dp": dp, "blk": lax.rem(b + p, 16)},
            device_id_type=pl.DeviceIdType.MESH,
        )
        return carry

    lax.fori_loop(1, 16, greet, 0)
    pl.semaphore_signal(
        barrier, inc=1, device_id=at(x, 3 - y, z), device_id_type=pl.DeviceIdType.MESH
    )

    used = [0, 0]
    to_finish = []

    def local(src, dst):
        copy = pltpu.make_async_copy(src, dst, s.local.at[used[1]])
        used[1] += 1
        copy.start()
        return copy

    def remote(src, dst, device, cond=None):
        n = used[0]
        used[0] += 1
        copy = pltpu.make_async_remote_copy(
            src_ref=src, dst_ref=dst, send_sem=s.send.at[n], recv_sem=s.recv.at[n],
            device_id=device, device_id_type=pl.DeviceIdType.MESH,
        )
        if cond is None:
            copy.start()
        else:
            @pl.when(cond)
            def _():
                copy.start()
        to_finish.append((copy, cond))
        return copy

    def arrived(copy, cond=None):
        if cond is None:
            copy.wait_recv()
        else:
            @pl.when(cond)
            def _():
                copy.wait_recv()

    wrapped = (b == 0) | (b == 15)
    sends_low_q = b >= 14
    sends_up_k = b >= 2
    plain = (b >= 1) & (b <= 14)

    load_cx = [local(ctx.at[:, cols[i]], s.cx.at[i]) for i in range(4)]
    load_go = [local(go.at[:, cols[i]], s.gox.at[i]) for i in range(4)]
    load_kv = []
    for i in range(4):
        load_kv.append(
            (
                local(k.at[:, cols[i]], s.kk.at[i, pl.ds(0, 256)]),
                local(v.at[:, cols[i]], s.vv.at[i, pl.ds(0, 256)]),
            )
        )
    load_gt = local(gout, s.gt.at[0])
    load_ly = local(lay, s.ly.at[0])
    load_g = []
    for i in range(4):
        load_g.append(
            (
                local(gq.at[:, cols[i]], s.gqs.at[i]),
                local(gk.at[:, cols[i]], s.gks.at[i]),
                local(gv.at[:, cols[i]], s.gvs.at[i]),
            )
        )

    own_docs = docs[...].astype(full)
    s.ds[...] = jnp.broadcast_to(own_docs, (8, 256))
    s.dk[pl.ds(0, 256), :] = jnp.transpose(jnp.broadcast_to(own_docs, (128, 256)))
    ones = jnp.ones((8, 256), low)
    for i in range(4):
        load_cx[i].wait()
        load_go[i].wait()
        product = s.cx[i].astype(full) * s.gox[i].astype(full)
        high_part = product.astype(low)
        low_part = (product - high_part.astype(full)).astype(low)
        row_dot = dot(ones, high_part, NT) + dot(ones, low_part, NT)
        s.meta[i, pl.ds(0, 1), :] = mass[pl.ds(heads[i], 1), :]
        s.meta[i, pl.ds(1, 1), :] = row_dot[0:1, :]
        s.meta[i, pl.ds(2, 1), :] = own_docs
        s.rtf_o[i, 0] = jnp.transpose(s.cx[i]).reshape(2, 2, 64, 256)

    @pl.when(wrapped)
    def _():
        for i in range(4):
            s.kk[i, pl.ds(384, 128), :] = jnp.zeros((128, 256), low)
            s.vv[i, pl.ds(384, 128), :] = jnp.zeros((128, 256), low)

    pl.semaphore_wait(barrier, 31)

    lower, upper = pl.ds(0, 128), pl.ds(128, 128)
    go_meta = remote(s.meta, s.mr, up_b)
    go_docs = remote(s.ds, s.dr, dn_b)
    send_rto = remote(s.rtf_o.at[:, :, :, 1 - c], s.rtp_o, mate)
    send_gt = remote(gout, s.gt.at[1], mate)
    forward = {}

    def send_forward(i):
        k_low = remote(k.at[lower, cols[i]], s.kk.at[i, pl.ds(256, 128)], dn_b)
        q_up = remote(q.at[upper, cols[i]], s.qr.at[i, 0], up_b)
        k_up = remote(k.at[upper, cols[i]], s.kk.at[i, pl.ds(384, 128)], dn_b, sends_up_k)
        q_low = remote(q.at[lower, cols[i]], s.qr.at[i, 1], up_b, sends_low_q)
        v_low = remote(v.at[lower, cols[i]], s.vv.at[i, pl.ds(256, 128)], dn_b)
        o_up = remote(go.at[upper, cols[i]], s.orr.at[i, 0], up_b)
        v_up = remote(v.at[upper, cols[i]], s.vv.at[i, pl.ds(384, 128)], dn_b, sends_up_k)
        o_low = remote(go.at[lower, cols[i]], s.orr.at[i, 1], up_b, sends_low_q)
        forward[i] = [
            (k_low, None), (q_up, None), (k_up, plain), (q_low, wrapped),
            (v_low, None), (o_up, None), (v_up, plain), (o_low, wrapped),
        ]

    send_forward(0)
    send_forward(1)
    send_ly = remote(lay, s.ly.at[1], mate)

    def weight_part(left, mate_left, right, p_ref, i, w):
        def block(db, carry):
            lanes = pl.ds(pl.multiple_of(db * 256, 256), 256)
            out = dot(left, right[0, :, lanes], NN) + dot(mate_left, right[1, :, lanes], NN)
            out = out.astype(low).reshape(-1, w, 2, 64, 256)
            y_hi = lax.div(db, 4)
            per_half = p_ref.shape[-1] // 256
            half = lax.div(lax.rem(db, 4), per_half)
            at_lane = pl.ds(pl.multiple_of(lax.rem(db, per_half) * 256, 256), 256)
            for n in range(out.shape[0]):
                for one in range(2):
                    p_ref[i + n, half, y_hi * 2 + one, :, :, at_lane] = out[n, :, one]
            return carry

        lax.fori_loop(0, 8, block, 0)

    def add_to(ref, *others):
        total = ref[...].astype(full)
        for other in others:
            total = total + other[...].astype(full)
        ref[...] = total.astype(low)

    top, bottom = pl.ds(0, 32), pl.ds(32, 32)

    class Group:
        def __init__(self, tag, w):
            self.w = w
            for name in ("p", "xa", "xb", "ya", "yb", "ea", "eb", "fa", "fb", "zs", "zr", "rtf", "rtp"):
                setattr(self, name, getattr(s, name + "_" + tag))
            self.ea_copy, self.eb_copy, self.xb_copy = {}, {}, {}
            self.index = 0 if tag == "o" else 1

        def x_first(self, i):
            p = self.p
            if i == 0:
                self.xa0 = remote(p.at[0, 0, pl.ds(0, 2)], self.xa.at[0], up_x)
                self.xa1 = remote(p.at[0, 0, pl.ds(2, 2)], self.xa.at[1], dn_x)
            elif i == 1:
                arrived(self.xa0)
                add_to(p.at[1, 0, pl.ds(0, 2)], self.xa.at[0])
                self.send_chunks(1, 0, up_x)
            elif i == 2:
                arrived(self.xa1)
                add_to(p.at[2, 0, pl.ds(2, 2)], self.xa.at[1])
                self.send_chunks(2, 1, dn_x)

        def send_chunks(self, i, way, device):
            self.xb_copy[way] = [
                remote(self.p.at[i, 0, chunk], self.xb.at[way, chunk], device)
                for chunk in (y_two, y_one, y_three, y)
            ]

        def take_chunk(self, n, chunk):
            arrived(self.xb_copy[0][n])
            arrived(self.xb_copy[1][n])
            return (self.xb.at[0, chunk], self.xb.at[1, chunk])

        def x_first_end(self):
            p = self.p
            add_to(p.at[3, 0, y_two], *self.take_chunk(0, y_two))
            self.ya0 = remote(p.at[3, 0, y_two, :, top], self.ya.at[0], up_y)
            self.ya1 = remote(p.at[3, 0, y_two, :, bottom], self.ya.at[1], dn_y)

        def then_y(self):
            p = self.p
            add_to(p.at[3, 0, y_one], *self.take_chunk(1, y_one))
            arrived(self.ya0)
            add_to(p.at[3, 0, y_one, :, top], self.ya.at[0])
            self.yb0 = remote(p.at[3, 0, y_one], self.yb.at[0], up_y)
            add_to(p.at[3, 0, y_three], *self.take_chunk(2, y_three))
            arrived(self.ya1)
            add_to(p.at[3, 0, y_three, :, bottom], self.ya.at[1])
            self.yb1 = remote(p.at[3, 0, y_three], self.yb.at[1], dn_y)

        def y_first(self, i):
            p = self.p
            self.ea_copy[i] = (
                remote(p.at[i, 1, y_two, :, top], self.ea.at[i, 0], up_y),
                remote(p.at[i, 1, y_two, :, bottom], self.ea.at[i, 1], dn_y),
            )

        def y_second(self, i):
            p = self.p
            arrived(self.ea_copy[i][0])
            add_to(p.at[i, 1, y_one, :, top], self.ea.at[i, 0])
            first = remote(p.at[i, 1, y_one], self.eb.at[i, 0], up_y)
            arrived(self.ea_copy[i][1])
            add_to(p.at[i, 1, y_three, :, bottom], self.ea.at[i, 1])
            self.eb_copy[i] = (first, remote(p.at[i, 1, y_three], self.eb.at[i, 1], dn_y))

        def y_end_then_x(self, i):
            p = self.p
            arrived(self.eb_copy[i][0])
            arrived(self.eb_copy[i][1])
            mine = p.at[i, 1, y]
            add_to(mine, self.eb.at[i, 0], self.eb.at[i, 1])
            if i == 0:
                self.fa0 = remote(p.at[0, 1, y, :, top], self.fa.at[0], up_x)
                self.fa1 = remote(p.at[0, 1, y, :, bottom], self.fa.at[1], dn_x)
            elif i == 1:
                arrived(self.fa0)
                add_to(p.at[1, 1, y, :, top], self.fa.at[0])
                self.fb0 = remote(mine, self.fb.at[0], up_x)
            elif i == 2:
                arrived(self.fa1)
                add_to(p.at[2, 1, y, :, bottom], self.fa.at[1])
                self.fb1 = remote(mine, self.fb.at[1], dn_x)

        def stage(self, mine, others, base):
            total = mine[...].astype(full)
            for other in others:
                total = total + other[...].astype(full)
            total = total.astype(low)
            pieces = total.shape[-1] // 128
            for n in range(pieces):
                self.zs[base + n] = total[:, :, n * 128 : (n + 1) * 128]
            for there in range(base, base + pieces):
                @pl.when(z != there)
                def _():
                    self.z_copy(there, lax.rem(there - z + 8, 8)).start()

        def z_copy(self, there, p):
            return pltpu.make_async_remote_copy(
                src_ref=self.zs.at[there], dst_ref=self.zr.at[p],
                send_sem=s.z_send.at[self.index, p], recv_sem=s.z_recv.at[self.index, p],
                device_id=at(x, y, there), device_id_type=pl.DeviceIdType.MESH,
            )

        def second_along_z(self):
            arrived(self.fb0)
            arrived(self.fb1)
            self.stage(self.p.at[3, 1, y], (self.fb.at[0], self.fb.at[1]), 4)

        def first_along_z(self):
            chunks = self.take_chunk(3, y)
            arrived(self.yb0)
            arrived(self.yb1)
            self.stage(self.p.at[3, 0, y], chunks + (self.yb.at[0], self.yb.at[1]), 0)

        def total(self):
            for p in range(1, 8):
                self.z_copy(lax.rem(z + p, 8), p).wait_recv()
            total = self.zs[z].astype(full)
            for p in range(1, 8):
                total = total + self.zr[p].astype(full)
            return total

        def finish(self):
            for p in range(1, 8):
                self.z_copy(lax.rem(z + p, 8), p).wait_send()

    out_g, main_g = Group("o", 1), Group("m", 3)

    load_gt.wait()
    arrived(send_rto)
    arrived(send_gt)
    weight_part(
        s.rtf_o[:, :, :, c].reshape(512, 256), s.rtp_o[...].reshape(512, 256), s.gt, s.p_o, 0, 1
    )
    out_g.x_first(0)

    j = lax.rem(b + 15, 16)
    halves_here = jnp.where(wrapped, 2, 1)
    row = lax.broadcasted_iota(jnp.int32, (512, 128), 0)
    key_block = jnp.where(row < 256, b, lax.rem(b + 1, 16))
    key_low = (row < 128) | ((row >= 256) & (row < 384))
    key_place = jnp.where(key_low, key_block, 31 - key_block)

    returns = {}

    def attention(i):
        for copy, cond in forward[i]:
            arrived(copy, cond)
        for copy in load_kv[i] + load_g[i]:
            copy.wait()
        s.acck[...] = jnp.zeros((256, 256), full)
        s.accv[...] = jnp.zeros((256, 256), full)

        def one_half(r, carry):
            lanes = pl.ds(pl.multiple_of((1 - r) * 128, 128), 128)
            query = s.qr[i, r]
            grad = s.orr[i, r]
            mass_row = s.mr[i, pl.ds(0, 1), lanes]
            dot_row = s.mr[i, pl.ds(1, 1), lanes]
            docs_row = s.mr[i, pl.ds(2, 1), lanes]
            place = jnp.where(r == 0, 31 - j, j)
            open_pairs = (s.dk[...] == docs_row) & (key_place < place)
            keys = s.kk[i]
            scores = dot(keys, query, NT) * SCALE
            scores = jnp.where(open_pairs, scores, -jnp.inf)
            peak = jnp.maximum(mass_row, jnp.max(scores, axis=0, keepdims=True))
            shifted = jnp.exp(scores - peak)
            norm = jnp.exp(mass_row - peak) + jnp.sum(shifted, axis=0, keepdims=True)
            attention_part = shifted * (1.0 / norm)
            grad_attention = dot(s.vv[i], grad, NT)
            grad_scores = (attention_part * (grad_attention - dot_row) * SCALE).astype(low)
            value_step = dot(attention_part.astype(low), grad, NN)
            key_step = dot(grad_scores, query, NN)
            s.gks[i] += key_step[0:256]
            s.gvs[i] += value_step[0:256]
            s.acck[...] += key_step[256:512]
            s.accv[...] += value_step[256:512]
            s.dqs[i, r] = dot(jnp.transpose(grad_scores), keys, NN).astype(low)
            return carry

        lax.fori_loop(0, halves_here, one_half, 0)
        s.dks[i] = s.acck[...].astype(low)
        s.dvs[i] = s.accv[...].astype(low)
        q_up = remote(s.dqs.at[i, 0], s.dqr.at[i, 0], dn_b)
        q_low = remote(s.dqs.at[i, 1], s.dqr.at[i, 1], dn_b, wrapped)
        k_low = remote(s.dks.at[i, lower], s.dkr.at[i, lower], up_b)
        k_up = remote(s.dks.at[i, upper], s.dkr.at[i, upper], up_b, plain)
        v_low = remote(s.dvs.at[i, lower], s.dvr.at[i, lower], up_b)
        v_up = remote(s.dvs.at[i, upper], s.dvr.at[i, upper], up_b, plain)
        returns[i] = [
            (q_up, None), (q_low, sends_low_q), (k_low, None),
            (k_up, sends_up_k), (v_low, None), (v_up, sends_up_k),
        ]

    exchanged = {}

    def finalize(i):
        for copy, cond in returns[i]:
            arrived(copy, cond)
        s.gqs[i, upper, :] += s.dqr[i, 0].astype(full)
        s.gks[i, lower, :] += s.dkr[i, lower, :].astype(full)
        s.gvs[i, lower, :] += s.dvr[i, lower, :].astype(full)

        @pl.when(sends_low_q)
        def _():
            s.gqs[i, lower, :] += s.dqr[i, 1].astype(full)

        @pl.when(sends_up_k)
        def _():
            s.gks[i, upper, :] += s.dkr[i, upper, :].astype(full)
            s.gvs[i, upper, :] += s.dvr[i, upper, :].astype(full)

        for w, total in enumerate((s.gqs, s.gks, s.gvs)):
            s.rtf_m[i, w] = jnp.transpose(total[i].astype(low)).reshape(2, 2, 64, 256)
        exchanged[i] = remote(s.rtf_m.at[i, :, :, 1 - c], s.rtp_m.at[i], mate)

    def weights_of(i):
        arrived(exchanged[i])
        weight_part(
            s.rtf_m[i, :, :, c].reshape(384, 256), s.rtp_m[i].reshape(384, 256), s.ly, s.p_m, i, 3
        )
        main_g.x_first(i)
        main_g.y_first(i)

    arrived(go_meta)
    arrived(go_docs)
    s.dk[pl.ds(256, 256), :] = jnp.transpose(jnp.broadcast_to(s.dr[0:1, :], (128, 256)))
    attention(0)
    send_forward(2)
    out_g.x_first(1)
    out_g.x_first(2)
    attention(1)
    send_forward(3)
    finalize(0)
    out_g.x_first_end()
    load_ly.wait()
    arrived(send_ly)
    attention(2)
    weights_of(0)
    finalize(1)
    out_g.then_y()
    attention(3)
    weights_of(1)
    main_g.y_second(0)
    finalize(2)
    out_g.first_along_z()
    weights_of(2)
    main_g.y_end_then_x(0)
    main_g.y_second(1)
    finalize(3)
    main_g.y_end_then_x(1)
    weights_of(3)
    main_g.y_second(2)
    main_g.x_first_end()
    main_g.y_end_then_x(2)
    main_g.y_second(3)
    main_g.then_y()
    main_g.y_end_then_x(3)
    main_g.second_along_z()
    main_g.first_along_z()
    s.grad[3] = out_g.total()[0] * (1.0 / ALL_TOKENS)
    s.grad[pl.ds(0, 3)] = main_g.total() * (1.0 / ALL_TOKENS)

    s.rows[...] = jnp.zeros((8, 128), full)
    s.cols[...] = jnp.zeros((8, 128), full)
    for w in range(4):
        squares = s.grad[w] * s.grad[w] + tiny_square
        s.rows[pl.ds(w, 1), :] = jnp.sum(squares, axis=0, keepdims=True)
        s.cols[pl.ds(w, 1), pl.ds(0, 64)] = jnp.sum(jnp.transpose(squares), axis=0, keepdims=True)
    s.rowr[pl.ds(0, 1)] = s.rows[...][None]
    s.colr[pl.ds(0, 1)] = s.cols[...][None]

    def stat_copy(src, dst, n, p, device):
        return pltpu.make_async_remote_copy(
            src_ref=src, dst_ref=dst, send_sem=s.stat_send.at[n, p], recv_sem=s.stat_recv.at[n, p],
            device_id=device, device_id_type=pl.DeviceIdType.MESH,
        )

    def row_copy(p):
        return stat_copy(s.rows, s.rowr.at[p], 0, p, {"dp": lax.rem(dp + p, 16), "blk": b})

    def col_copy(p):
        return stat_copy(s.cols, s.colr.at[p], 1, p, {"dp": dp, "blk": lax.rem(b + p, 16)})

    def tot_copy(p):
        return stat_copy(s.tot, s.totr.at[p], 2, p, {"dp": dp, "blk": lax.rem(b + p, 16)})

    def each(action):
        def step(p, carry):
            action(p)
            return carry

        lax.fori_loop(1, 16, step, 0)

    each(lambda p: row_copy(p).start())
    each(lambda p: col_copy(p).start())
    each(lambda p: row_copy(p).wait_recv())
    row_sum = jnp.sum(s.rowr[...], axis=0)[0:4]
    new_row = beta_two * rf[...] + (1.0 - beta_two) * (row_sum / 1024.0)
    orf[...] = new_row
    s.tot[...] = jnp.zeros((8, 128), full)
    s.tot[pl.ds(0, 4), :] = new_row
    s.totr[pl.ds(0, 1)] = s.tot[...][None]
    each(lambda p: tot_copy(p).start())
    each(lambda p: col_copy(p).wait_recv())
    col_sum = jnp.sum(s.colr[...], axis=0)[0:4, 0:64]
    new_col = beta_two * cf[...] + (1.0 - beta_two) * (col_sum / 2048.0)
    ocf[...] = new_col
    each(lambda p: tot_copy(p).wait_recv())
    all_rows = jnp.sum(s.totr[...], axis=0)[0:4]
    row_mean = jnp.sum(all_rows, axis=1, keepdims=True) / 2048.0
    for w in range(4):
        col_wide = jnp.transpose(jnp.broadcast_to(new_col[w : w + 1, :], (128, 64)))
        second = new_row[w : w + 1, :] * col_wide / row_mean[w : w + 1, :]
        ow[w] = wts[w] - learn_rate * s.grad[w] * lax.rsqrt(second)

    out_g.finish()
    main_g.finish()
    each(lambda p: row_copy(p).wait_send())
    each(lambda p: col_copy(p).wait_send())
    each(lambda p: tot_copy(p).wait_send())
    for copy, cond in to_finish:
        if cond is None:
            copy.wait_send()
        else:
            @pl.when(cond)
            def _(copy=copy):
                copy.wait_send()


def body(
    layer_input, queries, key_rows, value_rows, context, grad_context, grad_output, earlier_mass,
    grad_queries, grad_keys, grad_values, documents, weights, row_factor, column_factor,
):
    far = pl.BlockSpec(memory_space=pl.ANY)
    near = pl.BlockSpec(memory_space=pltpu.VMEM)
    new_weights, new_row, new_col = pl.pallas_call(
        kernel,
        out_shape=(
            jax.ShapeDtypeStruct((4, 64, 128), full),
            jax.ShapeDtypeStruct((4, 128), full),
            jax.ShapeDtypeStruct((4, 64), full),
        ),
        in_specs=[far] * 7 + [near] + [far] * 3 + [near] * 4,
        out_specs=(near, near, near),
        scratch_shapes=list(SCRATCH.values()),
        compiler_params=pltpu.CompilerParams(
            collective_id=0, has_side_effects=True, vmem_limit_bytes=60 * 1024 * 1024
        ),
    )(
        layer_input[0], queries[0], key_rows[0], value_rows[0], context[0], grad_context[0],
        grad_output[0], earlier_mass[0], grad_queries[0], grad_keys[0], grad_values[0], documents,
        jnp.transpose(weights, (0, 2, 1)), row_factor, column_factor,
    )
    return jnp.transpose(new_weights, (0, 2, 1)), new_row, new_col


def solution(mesh):
    placed = (P("dp", "blk", None),) * 7 + (P("dp", None, "blk"),) + (P("dp", "blk", None),) * 3 + (
        P("dp", "blk"),
        P(None, "blk", "dp"),
        P(None, "blk"),
        P(None, "dp"),
    )
    return jax.shard_map(
        body,
        mesh=mesh,
        in_specs=placed,
        out_specs=(P(None, "blk", "dp"), P(None, "blk"), P(None, "dp")),
        check_vma=False,
    )
```

```python
from types import SimpleNamespace

import jax
import jax.numpy as jnp
from jax import lax
from jax.experimental import pallas as pl
from jax.experimental.pallas import tpu as pltpu
from jax.sharding import PartitionSpec as P

beta_two = 0.9
learn_rate = 0.05
tiny_square = 1e-30
low = jnp.bfloat16
full = jnp.float32
ALL_TOKENS = 65536.0
SCALE = 1.0 / 16.0

NT = (((1,), (1,)), ((), ()))
NN = (((1,), (0,)), ((), ()))
TN = (((0,), (0,)), ((), ()))


def dot(a, b, dims):
    return lax.dot_general(a, b, dims, preferred_element_type=full)


def group_scratch(tag, w, lanes):
    return {
        "p_" + tag: pltpu.VMEM((4, 1024 // lanes, 4, w, 64, lanes), low),
        "xa_" + tag: pltpu.VMEM((2, 2, w, 64, lanes), low),
        "xb_" + tag: pltpu.VMEM((2, 4, w, 64, lanes), low),
        "ya_" + tag: pltpu.VMEM((2, w, 32, lanes), low),
        "yb_" + tag: pltpu.VMEM((2, w, 64, lanes), low),
        "ea_" + tag: pltpu.VMEM((4, 2, w, 32, 512), low),
        "eb_" + tag: pltpu.VMEM((4, 2, w, 64, 512), low),
        "fa_" + tag: pltpu.VMEM((2, w, 32, 512), low),
        "fb_" + tag: pltpu.VMEM((2, w, 64, 512), low),
        "zs_" + tag: pltpu.VMEM((8, w, 64, 128), low),
        "zr_" + tag: pltpu.VMEM((8, w, 64, 128), low),
        "rtf_" + tag: pltpu.VMEM((4, w, 2, 2, 64, 256), low),
        "rtp_" + tag: pltpu.VMEM((4, w, 2, 64, 256), low),
    }


N_SEM = 240
SCRATCH = {
    "ly": pltpu.VMEM((2, 256, 2048), low),
    "gt": pltpu.VMEM((2, 256, 2048), low),
    "cx": pltpu.VMEM((4, 256, 256), low),
    "gox": pltpu.VMEM((4, 256, 256), low),
    "kk": pltpu.VMEM((4, 512, 256), low),
    "vv": pltpu.VMEM((4, 512, 256), low),
    "qr": pltpu.VMEM((4, 2, 128, 256), low),
    "orr": pltpu.VMEM((4, 2, 128, 256), low),
    "gqs": pltpu.VMEM((4, 256, 256), full),
    "gks": pltpu.VMEM((4, 256, 256), full),
    "gvs": pltpu.VMEM((4, 256, 256), full),
    "meta": pltpu.VMEM((4, 8, 256), full),
    "mr": pltpu.VMEM((4, 8, 256), full),
    "ds": pltpu.VMEM((8, 256), full),
    "dr": pltpu.VMEM((8, 256), full),
    "dk": pltpu.VMEM((512, 128), full),
    "acck": pltpu.VMEM((256, 256), full),
    "accv": pltpu.VMEM((256, 256), full),
    "dqs": pltpu.VMEM((4, 2, 128, 256), low),
    "dks": pltpu.VMEM((4, 256, 256), low),
    "dvs": pltpu.VMEM((4, 256, 256), low),
    "dqr": pltpu.VMEM((4, 2, 128, 256), low),
    "dkr": pltpu.VMEM((4, 256, 256), low),
    "dvr": pltpu.VMEM((4, 256, 256), low),
    "rows": pltpu.VMEM((8, 128), full),
    "cols": pltpu.VMEM((8, 128), full),
    "tot": pltpu.VMEM((8, 128), full),
    "rowr": pltpu.VMEM((16, 8, 128), full),
    "colr": pltpu.VMEM((16, 8, 128), full),
    "totr": pltpu.VMEM((16, 8, 128), full),
    "grad": pltpu.VMEM((4, 64, 128), full),
    "z_send": pltpu.SemaphoreType.DMA((2, 8)),
    "z_recv": pltpu.SemaphoreType.DMA((2, 8)),
    **group_scratch("o", 1, 1024),
    **group_scratch("m", 3, 512),
    "send": pltpu.SemaphoreType.DMA((N_SEM,)),
    "recv": pltpu.SemaphoreType.DMA((N_SEM,)),
    "local": pltpu.SemaphoreType.DMA((40,)),
    "stat_send": pltpu.SemaphoreType.DMA((3, 16)),
    "stat_recv": pltpu.SemaphoreType.DMA((3, 16)),
}


def kernel(lay, q, k, v, ctx, go, gout, mass, gq, gk, gv, docs, wts, rf, cf, ow, orf, ocf, *scr):
    s = SimpleNamespace(**dict(zip(SCRATCH, scr)))
    dp = lax.axis_index("dp")
    b = lax.axis_index("blk")
    x = lax.div(dp, 4)
    yl = lax.rem(lax.div(dp, 2), 2)
    c = lax.rem(dp, 2)
    yh = lax.div(b, 8)
    z = lax.rem(b, 8)
    y = yh * 2 + yl

    def at(x_, y_, z_):
        return {"dp": x_ * 4 + lax.rem(y_, 2) * 2 + c, "blk": lax.div(y_, 2) * 8 + z_}

    up_x, dn_x = at(lax.rem(x + 1, 4), y, z), at(lax.rem(x + 3, 4), y, z)
    up_y, dn_y = at(x, lax.rem(y + 1, 4), z), at(x, lax.rem(y + 3, 4), z)
    y_one, y_two, y_three = lax.rem(y + 1, 4), lax.rem(y + 2, 4), lax.rem(y + 3, 4)
    mate = {"dp": dp + 1 - 2 * c, "blk": b}
    up_b, dn_b = {"dp": dp, "blk": lax.rem(b + 1, 16)}, {"dp": dp, "blk": lax.rem(b + 15, 16)}
    heads = [lax.rem(x + 2, 4), lax.rem(x + 1, 4), lax.rem(x + 3, 4), x]
    cols = [pl.ds(pl.multiple_of(h * 256, 256), 256) for h in heads]

    barrier = pltpu.get_barrier_semaphore()

    def greet(p, carry):
        pl.semaphore_signal(
            barrier, inc=1, device_id={"dp": lax.rem(dp + p, 16), "blk": b},
            device_id_type=pl.DeviceIdType.MESH,
        )
        pl.semaphore_signal(
            barrier, inc=1, device_id={"dp": dp, "blk": lax.rem(b + p, 16)},
            device_id_type=pl.DeviceIdType.MESH,
        )
        return carry

    lax.fori_loop(1, 16, greet, 0)
    pl.semaphore_signal(
        barrier, inc=1, device_id=at(x, 3 - y, z), device_id_type=pl.DeviceIdType.MESH
    )

    used = [0, 0]
    to_finish = []

    def local(src, dst):
        copy = pltpu.make_async_copy(src, dst, s.local.at[used[1]])
        used[1] += 1
        copy.start()
        return copy

    def remote(src, dst, device, cond=None):
        n = used[0]
        used[0] += 1
        copy = pltpu.make_async_remote_copy(
            src_ref=src, dst_ref=dst, send_sem=s.send.at[n], recv_sem=s.recv.at[n],
            device_id=device, device_id_type=pl.DeviceIdType.MESH,
        )
        if cond is None:
            copy.start()
        else:
            @pl.when(cond)
            def _():
                copy.start()
        to_finish.append((copy, cond))
        return copy

    def arrived(copy, cond=None):
        if cond is None:
            copy.wait_recv()
        else:
            @pl.when(cond)
            def _():
                copy.wait_recv()

    wrapped = (b == 0) | (b == 15)
    sends_low_q = b >= 14
    sends_up_k = b >= 2
    plain = (b >= 1) & (b <= 14)

    load_cx = [local(ctx.at[:, cols[i]], s.cx.at[i]) for i in range(4)]
    load_go = [local(go.at[:, cols[i]], s.gox.at[i]) for i in range(4)]
    load_kv = []
    for i in range(4):
        load_kv.append(
            (
                local(k.at[:, cols[i]], s.kk.at[i, pl.ds(0, 256)]),
                local(v.at[:, cols[i]], s.vv.at[i, pl.ds(0, 256)]),
            )
        )
    load_gt = local(gout, s.gt.at[0])
    load_ly = local(lay, s.ly.at[0])
    load_g = []
    for i in range(4):
        load_g.append(
            (
                local(gq.at[:, cols[i]], s.gqs.at[i]),
                local(gk.at[:, cols[i]], s.gks.at[i]),
                local(gv.at[:, cols[i]], s.gvs.at[i]),
            )
        )

    own_docs = docs[...].astype(full)
    s.ds[...] = jnp.broadcast_to(own_docs, (8, 256))
    s.dk[pl.ds(0, 256), :] = jnp.transpose(jnp.broadcast_to(own_docs, (128, 256)))
    ones = jnp.ones((8, 256), low)
    for i in range(4):
        load_cx[i].wait()
        load_go[i].wait()
        product = s.cx[i].astype(full) * s.gox[i].astype(full)
        high_part = product.astype(low)
        low_part = (product - high_part.astype(full)).astype(low)
        row_dot = dot(ones, high_part, NT) + dot(ones, low_part, NT)
        s.meta[i, pl.ds(0, 1), :] = mass[pl.ds(heads[i], 1), :]
        s.meta[i, pl.ds(1, 1), :] = row_dot[0:1, :]
        s.meta[i, pl.ds(2, 1), :] = own_docs
        s.rtf_o[i, 0] = jnp.transpose(s.cx[i]).reshape(2, 2, 64, 256)

    @pl.when(wrapped)
    def _():
        for i in range(4):
            s.kk[i, pl.ds(384, 128), :] = jnp.zeros((128, 256), low)
            s.vv[i, pl.ds(384, 128), :] = jnp.zeros((128, 256), low)

    pl.semaphore_wait(barrier, 31)

    lower, upper = pl.ds(0, 128), pl.ds(128, 128)
    go_meta = remote(s.meta, s.mr, up_b)
    go_docs = remote(s.ds, s.dr, dn_b)
    send_rto = remote(s.rtf_o.at[:, :, :, 1 - c], s.rtp_o, mate)
    send_gt = remote(gout, s.gt.at[1], mate)
    forward = {}

    def send_forward(i):
        k_low = remote(k.at[lower, cols[i]], s.kk.at[i, pl.ds(256, 128)], dn_b)
        q_up = remote(q.at[upper, cols[i]], s.qr.at[i, 0], up_b)
        k_up = remote(k.at[upper, cols[i]], s.kk.at[i, pl.ds(384, 128)], dn_b, sends_up_k)
        q_low = remote(q.at[lower, cols[i]], s.qr.at[i, 1], up_b, sends_low_q)
        v_low = remote(v.at[lower, cols[i]], s.vv.at[i, pl.ds(256, 128)], dn_b)
        o_up = remote(go.at[upper, cols[i]], s.orr.at[i, 0], up_b)
        v_up = remote(v.at[upper, cols[i]], s.vv.at[i, pl.ds(384, 128)], dn_b, sends_up_k)
        o_low = remote(go.at[lower, cols[i]], s.orr.at[i, 1], up_b, sends_low_q)
        forward[i] = [
            (k_low, None), (q_up, None), (k_up, plain), (q_low, wrapped),
            (v_low, None), (o_up, None), (v_up, plain), (o_low, wrapped),
        ]

    send_forward(0)
    send_forward(1)
    send_ly = remote(lay, s.ly.at[1], mate)

    def weight_part(left, mate_left, right, p_ref, i, w):
        def block(db, carry):
            lanes = pl.ds(pl.multiple_of(db * 256, 256), 256)
            out = dot(left, right[0, :, lanes], NN) + dot(mate_left, right[1, :, lanes], NN)
            out = out.astype(low).reshape(-1, w, 2, 64, 256)
            y_hi = lax.div(db, 4)
            per_half = p_ref.shape[-1] // 256
            half = lax.div(lax.rem(db, 4), per_half)
            at_lane = pl.ds(pl.multiple_of(lax.rem(db, per_half) * 256, 256), 256)
            for n in range(out.shape[0]):
                for one in range(2):
                    p_ref[i + n, half, y_hi * 2 + one, :, :, at_lane] = out[n, :, one]
            return carry

        lax.fori_loop(0, 8, block, 0)

    def add_to(ref, *others):
        total = ref[...].astype(full)
        for other in others:
            total = total + other[...].astype(full)
        ref[...] = total.astype(low)

    top, bottom = pl.ds(0, 32), pl.ds(32, 32)

    class Group:
        def __init__(self, tag, w):
            self.w = w
            for name in ("p", "xa", "xb", "ya", "yb", "ea", "eb", "fa", "fb", "zs", "zr", "rtf", "rtp"):
                setattr(self, name, getattr(s, name + "_" + tag))
            self.ea_copy, self.eb_copy, self.xb_copy = {}, {}, {}
            self.index = 0 if tag == "o" else 1

        def x_first(self, i):
            p = self.p
            if i == 0:
                self.xa0 = remote(p.at[0, 0, pl.ds(0, 2)], self.xa.at[0], up_x)
                self.xa1 = remote(p.at[0, 0, pl.ds(2, 2)], self.xa.at[1], dn_x)
            elif i == 1:
                arrived(self.xa0)
                add_to(p.at[1, 0, pl.ds(0, 2)], self.xa.at[0])
                self.send_chunks(1, 0, up_x)
            elif i == 2:
                arrived(self.xa1)
                add_to(p.at[2, 0, pl.ds(2, 2)], self.xa.at[1])
                self.send_chunks(2, 1, dn_x)

        def send_chunks(self, i, way, device):
            self.xb_copy[way] = [
                remote(self.p.at[i, 0, chunk], self.xb.at[way, chunk], device)
                for chunk in (y_two, y_one, y_three, y)
            ]

        def take_chunk(self, n, chunk):
            arrived(self.xb_copy[0][n])
            arrived(self.xb_copy[1][n])
            return (self.xb.at[0, chunk], self.xb.at[1, chunk])

        def x_first_end(self):
            p = self.p
            add_to(p.at[3, 0, y_two], *self.take_chunk(0, y_two))
            self.ya0 = remote(p.at[3, 0, y_two, :, top], self.ya.at[0], up_y)
            self.ya1 = remote(p.at[3, 0, y_two, :, bottom], self.ya.at[1], dn_y)

        def then_y(self):
            p = self.p
            add_to(p.at[3, 0, y_one], *self.take_chunk(1, y_one))
            arrived(self.ya0)
            add_to(p.at[3, 0, y_one, :, top], self.ya.at[0])
            self.yb0 = remote(p.at[3, 0, y_one], self.yb.at[0], up_y)
            add_to(p.at[3, 0, y_three], *self.take_chunk(2, y_three))
            arrived(self.ya1)
            add_to(p.at[3, 0, y_three, :, bottom], self.ya.at[1])
            self.yb1 = remote(p.at[3, 0, y_three], self.yb.at[1], dn_y)

        def y_first(self, i):
            p = self.p
            self.ea_copy[i] = (
                remote(p.at[i, 1, y_two, :, top], self.ea.at[i, 0], up_y),
                remote(p.at[i, 1, y_two, :, bottom], self.ea.at[i, 1], dn_y),
            )

        def y_second(self, i):
            p = self.p
            arrived(self.ea_copy[i][0])
            add_to(p.at[i, 1, y_one, :, top], self.ea.at[i, 0])
            first = remote(p.at[i, 1, y_one], self.eb.at[i, 0], up_y)
            arrived(self.ea_copy[i][1])
            add_to(p.at[i, 1, y_three, :, bottom], self.ea.at[i, 1])
            self.eb_copy[i] = (first, remote(p.at[i, 1, y_three], self.eb.at[i, 1], dn_y))

        def y_end_then_x(self, i):
            p = self.p
            arrived(self.eb_copy[i][0])
            arrived(self.eb_copy[i][1])
            mine = p.at[i, 1, y]
            add_to(mine, self.eb.at[i, 0], self.eb.at[i, 1])
            if i == 0:
                self.fa0 = remote(p.at[0, 1, y, :, top], self.fa.at[0], up_x)
                self.fa1 = remote(p.at[0, 1, y, :, bottom], self.fa.at[1], dn_x)
            elif i == 1:
                arrived(self.fa0)
                add_to(p.at[1, 1, y, :, top], self.fa.at[0])
                self.fb0 = remote(mine, self.fb.at[0], up_x)
            elif i == 2:
                arrived(self.fa1)
                add_to(p.at[2, 1, y, :, bottom], self.fa.at[1])
                self.fb1 = remote(mine, self.fb.at[1], dn_x)

        def stage(self, mine, others, base):
            total = mine[...].astype(full)
            for other in others:
                total = total + other[...].astype(full)
            total = total.astype(low)
            pieces = total.shape[-1] // 128
            for n in range(pieces):
                self.zs[base + n] = total[:, :, n * 128 : (n + 1) * 128]
            for there in range(base, base + pieces):
                @pl.when(z != there)
                def _():
                    self.z_copy(there, lax.rem(there - z + 8, 8)).start()

        def z_copy(self, there, p):
            return pltpu.make_async_remote_copy(
                src_ref=self.zs.at[there], dst_ref=self.zr.at[p],
                send_sem=s.z_send.at[self.index, p], recv_sem=s.z_recv.at[self.index, p],
                device_id=at(x, y, there), device_id_type=pl.DeviceIdType.MESH,
            )

        def second_along_z(self):
            arrived(self.fb0)
            arrived(self.fb1)
            self.stage(self.p.at[3, 1, y], (self.fb.at[0], self.fb.at[1]), 4)

        def first_along_z(self):
            chunks = self.take_chunk(3, y)
            arrived(self.yb0)
            arrived(self.yb1)
            self.stage(self.p.at[3, 0, y], chunks + (self.yb.at[0], self.yb.at[1]), 0)

        def total(self):
            for p in range(1, 8):
                self.z_copy(lax.rem(z + p, 8), p).wait_recv()
            total = self.zs[z].astype(full)
            for p in range(1, 8):
                total = total + self.zr[p].astype(full)
            return total

        def finish(self):
            for p in range(1, 8):
                self.z_copy(lax.rem(z + p, 8), p).wait_send()

    out_g, main_g = Group("o", 1), Group("m", 3)

    load_gt.wait()
    arrived(send_rto)
    arrived(send_gt)
    weight_part(
        s.rtf_o[:, :, :, c].reshape(512, 256), s.rtp_o[...].reshape(512, 256), s.gt, s.p_o, 0, 1
    )
    out_g.x_first(0)

    j = lax.rem(b + 15, 16)
    halves_here = jnp.where(wrapped, 2, 1)
    row = lax.broadcasted_iota(jnp.int32, (512, 128), 0)
    key_block = jnp.where(row < 256, b, lax.rem(b + 1, 16))
    key_low = (row < 128) | ((row >= 256) & (row < 384))
    key_place = jnp.where(key_low, key_block, 31 - key_block)

    returns = {}

    def attention(i):
        for copy, cond in forward[i]:
            arrived(copy, cond)
        for copy in load_kv[i] + load_g[i]:
            copy.wait()
        s.acck[...] = jnp.zeros((256, 256), full)
        s.accv[...] = jnp.zeros((256, 256), full)

        def one_half(r, carry):
            lanes = pl.ds(pl.multiple_of((1 - r) * 128, 128), 128)
            query = s.qr[i, r]
            grad = s.orr[i, r]
            mass_row = s.mr[i, pl.ds(0, 1), lanes]
            dot_row = s.mr[i, pl.ds(1, 1), lanes]
            docs_row = s.mr[i, pl.ds(2, 1), lanes]
            place = jnp.where(r == 0, 31 - j, j)
            open_pairs = (s.dk[...] == docs_row) & (key_place < place)
            keys = s.kk[i]
            scores = dot(keys, query, NT) * SCALE
            scores = jnp.where(open_pairs, scores, -jnp.inf)
            peak = jnp.maximum(mass_row, jnp.max(scores, axis=0, keepdims=True))
            shifted = jnp.exp(scores - peak)
            norm = jnp.exp(mass_row - peak) + jnp.sum(shifted, axis=0, keepdims=True)
            attention_part = shifted * (1.0 / norm)
            grad_attention = dot(s.vv[i], grad, NT)
            grad_scores = (attention_part * (grad_attention - dot_row) * SCALE).astype(low)
            value_step = dot(attention_part.astype(low), grad, NN)
            key_step = dot(grad_scores, query, NN)
            s.gks[i] += key_step[0:256]
            s.gvs[i] += value_step[0:256]
            s.acck[...] += key_step[256:512]
            s.accv[...] += value_step[256:512]
            s.dqs[i, r] = dot(jnp.transpose(grad_scores), keys, NN).astype(low)
            return carry

        lax.fori_loop(0, halves_here, one_half, 0)
        s.dks[i] = s.acck[...].astype(low)
        s.dvs[i] = s.accv[...].astype(low)
        q_up = remote(s.dqs.at[i, 0], s.dqr.at[i, 0], dn_b)
        q_low = remote(s.dqs.at[i, 1], s.dqr.at[i, 1], dn_b, wrapped)
        k_low = remote(s.dks.at[i, lower], s.dkr.at[i, lower], up_b)
        k_up = remote(s.dks.at[i, upper], s.dkr.at[i, upper], up_b, plain)
        v_low = remote(s.dvs.at[i, lower], s.dvr.at[i, lower], up_b)
        v_up = remote(s.dvs.at[i, upper], s.dvr.at[i, upper], up_b, plain)
        returns[i] = [
            (q_up, None), (q_low, sends_low_q), (k_low, None),
            (k_up, sends_up_k), (v_low, None), (v_up, sends_up_k),
        ]

    exchanged = {}

    def finalize(i):
        for copy, cond in returns[i]:
            arrived(copy, cond)
        s.gqs[i, upper, :] += s.dqr[i, 0].astype(full)
        s.gks[i, lower, :] += s.dkr[i, lower, :].astype(full)
        s.gvs[i, lower, :] += s.dvr[i, lower, :].astype(full)

        @pl.when(sends_low_q)
        def _():
            s.gqs[i, lower, :] += s.dqr[i, 1].astype(full)

        @pl.when(sends_up_k)
        def _():
            s.gks[i, upper, :] += s.dkr[i, upper, :].astype(full)
            s.gvs[i, upper, :] += s.dvr[i, upper, :].astype(full)

        for w, total in enumerate((s.gqs, s.gks, s.gvs)):
            s.rtf_m[i, w] = jnp.transpose(total[i].astype(low)).reshape(2, 2, 64, 256)
        exchanged[i] = remote(s.rtf_m.at[i, :, :, 1 - c], s.rtp_m.at[i], mate)

    def weights_of(i):
        arrived(exchanged[i])
        weight_part(
            s.rtf_m[i, :, :, c].reshape(384, 256), s.rtp_m[i].reshape(384, 256), s.ly, s.p_m, i, 3
        )
        main_g.x_first(i)
        if i > 1:
            main_g.y_first(i)

    arrived(go_meta)
    arrived(go_docs)
    s.dk[pl.ds(256, 256), :] = jnp.transpose(jnp.broadcast_to(s.dr[0:1, :], (128, 256)))
    attention(0)
    send_forward(2)
    out_g.x_first(1)
    out_g.x_first(2)
    attention(1)
    send_forward(3)
    finalize(0)
    load_ly.wait()
    arrived(send_ly)
    attention(2)
    weights_of(0)
    finalize(1)
    out_g.x_first_end()
    attention(3)
    weights_of(1)
    finalize(2)
    main_g.y_first(0)
    main_g.y_first(1)
    out_g.then_y()
    weights_of(2)
    main_g.y_second(0)
    main_g.y_second(1)
    finalize(3)
    main_g.y_end_then_x(0)
    weights_of(3)
    main_g.y_end_then_x(1)
    out_g.first_along_z()
    main_g.y_second(2)
    main_g.x_first_end()
    main_g.y_end_then_x(2)
    main_g.y_second(3)
    main_g.then_y()
    main_g.y_end_then_x(3)
    main_g.second_along_z()
    main_g.first_along_z()
    s.grad[3] = out_g.total()[0] * (1.0 / ALL_TOKENS)
    s.grad[pl.ds(0, 3)] = main_g.total() * (1.0 / ALL_TOKENS)

    s.rows[...] = jnp.zeros((8, 128), full)
    s.cols[...] = jnp.zeros((8, 128), full)
    for w in range(4):
        squares = s.grad[w] * s.grad[w] + tiny_square
        s.rows[pl.ds(w, 1), :] = jnp.sum(squares, axis=0, keepdims=True)
        s.cols[pl.ds(w, 1), pl.ds(0, 64)] = jnp.sum(jnp.transpose(squares), axis=0, keepdims=True)
    s.rowr[pl.ds(0, 1)] = s.rows[...][None]
    s.colr[pl.ds(0, 1)] = s.cols[...][None]

    def stat_copy(src, dst, n, p, device):
        return pltpu.make_async_remote_copy(
            src_ref=src, dst_ref=dst, send_sem=s.stat_send.at[n, p], recv_sem=s.stat_recv.at[n, p],
            device_id=device, device_id_type=pl.DeviceIdType.MESH,
        )

    def row_copy(p):
        return stat_copy(s.rows, s.rowr.at[p], 0, p, {"dp": lax.rem(dp + p, 16), "blk": b})

    def col_copy(p):
        return stat_copy(s.cols, s.colr.at[p], 1, p, {"dp": dp, "blk": lax.rem(b + p, 16)})

    def tot_copy(p):
        return stat_copy(s.tot, s.totr.at[p], 2, p, {"dp": dp, "blk": lax.rem(b + p, 16)})

    def each(action):
        def step(p, carry):
            action(p)
            return carry

        lax.fori_loop(1, 16, step, 0)

    each(lambda p: row_copy(p).start())
    each(lambda p: col_copy(p).start())
    each(lambda p: row_copy(p).wait_recv())
    row_sum = jnp.sum(s.rowr[...], axis=0)[0:4]
    new_row = beta_two * rf[...] + (1.0 - beta_two) * (row_sum / 1024.0)
    orf[...] = new_row
    s.tot[...] = jnp.zeros((8, 128), full)
    s.tot[pl.ds(0, 4), :] = new_row
    s.totr[pl.ds(0, 1)] = s.tot[...][None]
    each(lambda p: tot_copy(p).start())
    each(lambda p: col_copy(p).wait_recv())
    col_sum = jnp.sum(s.colr[...], axis=0)[0:4, 0:64]
    new_col = beta_two * cf[...] + (1.0 - beta_two) * (col_sum / 2048.0)
    ocf[...] = new_col
    each(lambda p: tot_copy(p).wait_recv())
    all_rows = jnp.sum(s.totr[...], axis=0)[0:4]
    row_mean = jnp.sum(all_rows, axis=1, keepdims=True) / 2048.0
    for w in range(4):
        col_wide = jnp.transpose(jnp.broadcast_to(new_col[w : w + 1, :], (128, 64)))
        second = new_row[w : w + 1, :] * col_wide / row_mean[w : w + 1, :]
        ow[w] = wts[w] - learn_rate * s.grad[w] * lax.rsqrt(second)

    out_g.finish()
    main_g.finish()
    each(lambda p: row_copy(p).wait_send())
    each(lambda p: col_copy(p).wait_send())
    each(lambda p: tot_copy(p).wait_send())
    for copy, cond in to_finish:
        if cond is None:
            copy.wait_send()
        else:
            @pl.when(cond)
            def _(copy=copy):
                copy.wait_send()


def body(
    layer_input, queries, key_rows, value_rows, context, grad_context, grad_output, earlier_mass,
    grad_queries, grad_keys, grad_values, documents, weights, row_factor, column_factor,
):
    far = pl.BlockSpec(memory_space=pl.ANY)
    near = pl.BlockSpec(memory_space=pltpu.VMEM)
    new_weights, new_row, new_col = pl.pallas_call(
        kernel,
        out_shape=(
            jax.ShapeDtypeStruct((4, 64, 128), full),
            jax.ShapeDtypeStruct((4, 128), full),
            jax.ShapeDtypeStruct((4, 64), full),
        ),
        in_specs=[far] * 7 + [near] + [far] * 3 + [near] * 4,
        out_specs=(near, near, near),
        scratch_shapes=list(SCRATCH.values()),
        compiler_params=pltpu.CompilerParams(
            collective_id=0, has_side_effects=True, vmem_limit_bytes=60 * 1024 * 1024
        ),
    )(
        layer_input[0], queries[0], key_rows[0], value_rows[0], context[0], grad_context[0],
        grad_output[0], earlier_mass[0], grad_queries[0], grad_keys[0], grad_values[0], documents,
        jnp.transpose(weights, (0, 2, 1)), row_factor, column_factor,
    )
    return jnp.transpose(new_weights, (0, 2, 1)), new_row, new_col


def solution(mesh):
    placed = (P("dp", "blk", None),) * 7 + (P("dp", None, "blk"),) + (P("dp", "blk", None),) * 3 + (
        P("dp", "blk"),
        P(None, "blk", "dp"),
        P(None, "blk"),
        P(None, "dp"),
    )
    return jax.shard_map(
        body,
        mesh=mesh,
        in_specs=placed,
        out_specs=(P(None, "blk", "dp"), P(None, "blk"), P(None, "dp")),
        check_vma=False,
    )
```
